32 devices in a mesh: dp: 8 (over y, x, core), expert: 4 (over z).
Axes of the slice: x: 2, y: 2, z: 4, core: 2. Of those that a mesh axis runs over, the one named last changes fastest.
Arguments:
- tokens: bfloat16 [512, 4096], P('expert', 'dp'), may hold values from -6 to 6
- in_signs: int32 [512, 128], P('expert', 'dp'), may hold values from -2147483648 to 2147483646
- out_signs: int32 [512, 224], P('expert'), may hold values from -2147483648 to 2147483646
- expert_ids: int32 [512, 2], P('expert'), may hold values from 0 to 3, all different within a row; in each aligned block of 128 rows (0 to 127, 128 to 255, ...) at most 80 rows name the same one
- route_weight: float32 [512, 2], P('expert'), may hold values from 0.2 to 1
- cotangent: bfloat16 [512, 7168], P('expert', 'dp'), may hold values from -6 to 6
- mean_weight: bfloat16 [4, 4096, 7168], P('expert', 'dp'), may hold values from -0.09375 to 0.09375
- rho_weight: bfloat16 [4, 4096, 7168], P('expert', 'dp'), may hold values from -6 to -3
- noise_weight: bfloat16 [4, 4096, 7168], P('expert', 'dp'), may hold values from -4 to 4
Outputs:
- hidden_out: bfloat16 [512, 7168], P('expert', 'dp')
- grad_tokens: bfloat16 [512, 4096], P('expert', 'dp')
- grad_mean: bfloat16 [4, 4096, 7168], P('expert', 'dp')
- grad_rho: bfloat16 [4, 4096, 7168], P('expert', 'dp')
The draws below stay inside these ranges and needn't reach their ends.
Inputs may be any that keep to these rules, and one draw needn't show every extreme that they name: `expert_ids`: each token names 2 different experts. In each aligned block of 128 tokens no expert is named by more than 80 tokens, and in some blocks one expert is named by exactly 80. `in_signs`: bit b of word w, counted from the lowest, is set where the sign of feature 32 * w + b is -1 and clear where it is +1. `out_signs`: bit b of word w, counted from the lowest, is set where the sign of hidden unit 32 * w + b is -1 and clear where it is +1.
All inputs are finite; a program needn't handle non-finite values.
Results may differ from the reference program's by a relative error of at most 0.0071.
Values may be sent and summed in bfloat16 or wider, within the bound.
A program may use at most 128 MiB of HBM per device.

```python
import math
import jax
import jax.numpy as jnp
import numpy as np
from jax import lax

D = 4096
FF = 7168
TOPK = 2
TOK_DEV = 128
EXPERTS = 4
CAP = 80
TOKENS = 512
N_EXPERT = 4


def with_ends(array, stream_key, low, top_value):
    shape = array.shape
    index_at = [jax.random.randint(jax.random.fold_in(stream_key, axis), (), 0, shape[axis]) for axis in range(len(shape))]
    array = array.at[tuple(index_at)].set(low)
    longest = shape.index(max(shape))
    index_at[longest] = (index_at[longest] + 1) % shape[longest]
    return array.at[tuple(index_at)].set(top_value)


def block_scale(rng, extent, pieces, least, high):
    def one(axis_at, blocks):
        steps = jax.random.uniform(jax.random.fold_in(jax.random.fold_in(rng, 6), axis_at), (blocks,), jnp.float32, least / len(pieces), high / len(pieces))
        return jnp.repeat(jnp.exp(steps), extent[axis_at] // blocks).reshape((-1,) + (1,) * (len(extent) - axis_at - 1))

    loudness = one(*pieces[0])
    for cut in pieces[1:]:
        loudness = loudness * one(*cut)
    return loudness


def shared_out(key, own, number, rows, number_of, top, limit, skew):
    ranking = jax.random.permutation(key, number_of)
    heavy_load, common = shares(number_of, rows * top, limit, skew, True), shares(number_of, rows * top, limit, skew, False)
    places = jnp.arange(number_of)

    def named(sizes, turn):
        used = int((sizes > 0).sum())
        fixed = max(1, used // 4)
        moved = fixed + (places - fixed + turn * (used - fixed)) % max(1, number_of - fixed)
        return jnp.zeros((number_of,), jnp.int32).at[ranking[jnp.where(places < fixed, places, moved)]].set(jnp.asarray(sizes, jnp.int32))

    sizes = jnp.where(number % 4 == 0, named(heavy_load, number // 4), named(common, number - number // 4 - 1))
    mixed = jax.random.permutation(jax.random.fold_in(own, 3), number_of)
    giver, sink = mixed[0:number_of // 2 * 2:2], mixed[1:number_of // 2 * 2:2]
    slack = jnp.minimum(sizes[giver] - 1, limit - sizes[sink]) // 2
    slack = jnp.where((giver == ranking[0]) | (sink == ranking[0]) | (sizes[sink] == 0), 0, jnp.maximum(slack, 0))
    moved = jax.random.randint(jax.random.fold_in(own, 4), (number_of // 2,), 0, 1 << 20) % (slack + 1)
    sizes = sizes.at[giver].add(-moved).at[sink].add(moved)
    members = jnp.searchsorted(jnp.cumsum(sizes), jnp.arange(rows * top), side="right").astype(jnp.int32)
    listing = members.reshape(top, rows).T
    listing = listing[jax.random.permutation(jax.random.fold_in(own, 1), rows)]
    turn = jax.random.randint(jax.random.fold_in(own, 2), (rows, 1), 0, top)
    return jnp.take_along_axis(listing, (jnp.arange(top)[None, :] + turn) % top, axis=1)


def shares(count, total, limit, skew, full):
    weights = [(1 << 20) // math.isqrt(grade ** skew) + 1 for grade in range(1, count + 1)]
    largest = limit if full else min(limit, max(-(-total // count), total * weights[0] // sum(weights)))
    least = 1 if total - largest >= count - 1 else 0
    holding, surplus = [largest] + [least] * (count - 1), total - largest - least * (count - 1)
    while surplus > 0:
        free = [i for i in range(1, count) if holding[i] < largest] or [i for i in range(1, count) if holding[i] < limit]
        whole, remaining = sum([weights[i] for i in free]), surplus
        for i in free:
            more = min(limit - holding[i], max(1, remaining * weights[i] // whole), surplus)
            holding[i] = holding[i] + more
            surplus = surplus - more
    return np.array(holding)


def bell_draw(key, dims, deviation, most, cuts=(), kind=jnp.bfloat16):
    entries = jax.random.normal(key, dims, jnp.float32) * deviation
    if len(cuts) > 0:
        entries = block_scale(key, dims, cuts, -0.22, 0.18) * entries
    return jnp.clip(entries, min=-most, max=most).astype(kind)


def setup_inputs(seed: int = 0) -> dict:
    key_list = jax.random.split(jax.random.key(seed), 10)
    tokens = bell_draw(key_list[0], (TOKENS, D), 1.0, 6.0, ((0, 4), (1, 8)))
    in_signs = with_ends(jax.random.randint(key_list[1], (TOKENS, D // 32), -2147483648, 2147483647), jax.random.fold_in(key_list[1], 1), -2147483648, 2147483646).astype(jnp.int32)
    out_signs = with_ends(jax.random.randint(key_list[2], (TOKENS, FF // 32), -2147483648, 2147483647), jax.random.fold_in(key_list[2], 1), -2147483648, 2147483646).astype(jnp.int32)
    expert_ids_keys = jax.random.split(jax.random.fold_in(key_list[3], 1), TOKENS // TOK_DEV)
    expert_ids_turns = jax.random.permutation(jax.random.fold_in(key_list[3], 3), TOKENS // TOK_DEV)
    expert_ids = jax.vmap(lambda own, number: shared_out(jax.random.fold_in(key_list[3], 2), own, number, TOK_DEV, EXPERTS, TOPK, CAP, 2))(expert_ids_keys, expert_ids_turns).reshape((TOKENS, TOPK))
    route_weight = jnp.clip(0.2 + 0.8 * jax.random.uniform(key_list[4], (TOKENS, TOPK), jnp.float32) ** block_scale(key_list[4], (TOKENS, TOPK), ((0, 4),), -0.2, 0.2), 0.2, 1.0)
    cotangent = bell_draw(key_list[5], (TOKENS, FF), 1.0, 6.0, ((0, 4), (1, 8)))
    mean_weight = bell_draw(key_list[6], (EXPERTS, D, FF), D ** -0.5, 0.09375, ((0, 4), (1, 8)))
    rho_weight = jnp.clip(-6.0 + 3.0 * jax.random.uniform(key_list[7], (EXPERTS, D, FF), jnp.float32) ** block_scale(key_list[7], (EXPERTS, D, FF), ((0, 4), (1, 8)), -0.2, 0.2), -6.0, -3.0).astype(jnp.bfloat16)
    noise_weight = bell_draw(key_list[8], (EXPERTS, D, FF), 1.0, 4.0, ((0, 4), (1, 8)))
    return dict(tokens=tokens, in_signs=in_signs, out_signs=out_signs, expert_ids=expert_ids, route_weight=route_weight, cotangent=cotangent, mean_weight=mean_weight, rho_weight=rho_weight, noise_weight=noise_weight)


def unpack_rows(words):
    shifts = jnp.arange(32, dtype=jnp.int32)
    bits = jnp.bitwise_and(jnp.right_shift(words[..., None], shifts), 1)
    signs = (1 - 2 * bits).astype(jnp.float32)
    return signs.reshape(words.shape[:-1] + (words.shape[-1] * 32,))


def block_slots(block_ids):
    onehot = (block_ids[:, :, None] == jnp.arange(EXPERTS, dtype=jnp.int32)).astype(jnp.int32)
    flat = onehot.reshape(-1, EXPERTS)
    before = (jnp.cumsum(flat, axis=0) - flat).astype(jnp.int32)
    return jnp.sum(before * flat, axis=1).astype(jnp.int32).reshape(block_ids.shape)


def reference(tokens, in_signs, out_signs, expert_ids, route_weight, cotangent, mean_weight, rho_weight, noise_weight):
    blocks = expert_ids.reshape(N_EXPERT, TOK_DEV, TOPK)
    ranks = jax.vmap(block_slots)(blocks)
    source = jnp.arange(N_EXPERT, dtype=jnp.int32)[:, None, None]
    per_expert = N_EXPERT * CAP
    position = (blocks * per_expert + source * CAP + ranks).astype(jnp.int32).reshape(TOKENS, TOPK)
    total = EXPERTS * per_expert
    token_index = jnp.broadcast_to(jnp.arange(TOKENS, dtype=jnp.int32)[:, None], (TOKENS, TOPK))
    flat_pos = position.reshape(-1)
    slot_token = jnp.zeros((total,), jnp.int32).at[flat_pos].set(token_index.reshape(-1))
    slot_fill = jnp.zeros((total,), jnp.float32).at[flat_pos].set(1.0)
    slot_weight = jnp.zeros((total,), jnp.float32).at[flat_pos].set(route_weight.reshape(-1))
    input_full = unpack_rows(in_signs)
    output_full = unpack_rows(out_signs)

    def one_expert(operands):
        mean_e, rho_e, noise_e, tok_e, fill_e, weight_e = operands
        rows = jnp.take(tokens, tok_e, axis=0) * fill_e[:, None].astype(jnp.bfloat16)
        input_rows = jnp.take(input_full, tok_e, axis=0)
        output_rows = jnp.take(output_full, tok_e, axis=0)
        signed = rows * input_rows.astype(jnp.bfloat16)
        rho_float = rho_e.astype(jnp.float32)
        noise_float = noise_e.astype(jnp.float32)
        delta = (jax.nn.softplus(rho_float) * noise_float).astype(jnp.bfloat16)
        mean_part = jnp.dot(rows, mean_e, preferred_element_type=jnp.float32)
        pert_part = jnp.dot(signed, delta, preferred_element_type=jnp.float32)
        preact = mean_part + output_rows * pert_part
        gate = jax.nn.sigmoid(preact)
        hidden = (preact * gate).astype(jnp.bfloat16)
        upstream = (jnp.take(cotangent, tok_e, axis=0).astype(jnp.float32) * weight_e[:, None]).astype(jnp.bfloat16)
        slope = gate * (1.0 + preact * (1.0 - gate))
        grad_preact = (upstream.astype(jnp.float32) * slope).astype(jnp.bfloat16)
        grad_signed_pre = grad_preact * output_rows.astype(jnp.bfloat16)
        grad_mean_e = jnp.dot(rows.T, grad_preact, preferred_element_type=jnp.float32).astype(jnp.bfloat16)
        grad_delta = jnp.dot(signed.T, grad_signed_pre, preferred_element_type=jnp.float32)
        grad_rho_e = (grad_delta * noise_float * jax.nn.sigmoid(rho_float)).astype(jnp.bfloat16)
        back = jnp.dot(grad_preact, mean_e.T, preferred_element_type=jnp.float32)
        back = back + input_rows * jnp.dot(grad_signed_pre, delta.T, preferred_element_type=jnp.float32)
        return hidden, back.astype(jnp.bfloat16), grad_mean_e, grad_rho_e

    operands = (mean_weight, rho_weight, noise_weight, slot_token.reshape(EXPERTS, per_expert),
                slot_fill.reshape(EXPERTS, per_expert), slot_weight.reshape(EXPERTS, per_expert))
    hidden_slots, back_slots, grad_mean, grad_rho = lax.map(one_expert, operands)
    picked = jnp.take(hidden_slots.reshape(total, FF), position, axis=0).astype(jnp.float32)
    hidden_out = jnp.sum(picked * route_weight[:, :, None], axis=1).astype(jnp.bfloat16)
    returned = jnp.take(back_slots.reshape(total, D), position, axis=0).astype(jnp.float32)
    grad_tokens = jnp.sum(returned, axis=1).astype(jnp.bfloat16)
    return hidden_out, grad_tokens, grad_mean, grad_rho
```

```python
import functools

import jax
import jax.numpy as jnp
from jax import lax
from jax.experimental import pallas as pl
from jax.experimental.pallas import tpu as pltpu
from jax.sharding import PartitionSpec as P

def unpack_rows(words):
    shifts = jnp.arange(32, dtype=jnp.int32)
    bits = jnp.bitwise_and(jnp.right_shift(words[..., None], shifts), 1)
    signs = (1 - 2 * bits).astype(jnp.float32)
    return signs.reshape(words.shape[:-1] + (words.shape[-1] * 32,))


def unpack_cols(words):
    shifts = jnp.arange(32, dtype=jnp.int32)
    bits = jnp.bitwise_and(jnp.right_shift(words.T[:, None, :], shifts[None, :, None]), 1)
    signs = (1 - 2 * bits).astype(jnp.float32)
    return signs.reshape(words.shape[1] * 32, words.shape[0])


def block_slots(block_ids, experts, capacity):
    onehot = (block_ids[:, :, None] == jnp.arange(experts, dtype=jnp.int32)).astype(jnp.int32)
    flat = onehot.reshape(-1, experts)
    before = jnp.cumsum(flat, axis=0) - flat
    ranks = jnp.sum(before * flat, axis=1).reshape(block_ids.shape)
    return block_ids * capacity + ranks


def on_device_general(
    tokens,
    in_signs,
    out_signs,
    expert_ids,
    route_weight,
    cotangent,
    mean_weight,
    rho_weight,
    noise_weight,
):
    experts = lax.axis_size("expert") * mean_weight.shape[0]
    token_count = tokens.shape[0]
    topk = expert_ids.shape[1]
    capacity = 5 * token_count * topk // (4 * experts)
    slots = experts * capacity
    width_local = tokens.shape[1]
    sign_words = in_signs.shape[1]
    hidden_local = cotangent.shape[1]
    slot_of = block_slots(expert_ids, experts, capacity)
    match = (slot_of[:, :, None] == jnp.arange(slots, dtype=jnp.int32)).astype(jnp.int32)
    token_rank = jnp.arange(token_count, dtype=jnp.int32)[:, None, None]
    slot_token = jnp.sum(match * token_rank, axis=(0, 1))
    slot_fill = jnp.sum(match, axis=(0, 1))
    slot_weight = jnp.sum(match.astype(jnp.float32) * route_weight[:, :, None], axis=(0, 1))
    words = jnp.concatenate([in_signs, out_signs], axis=1)
    fill_rows = slot_fill.astype(jnp.bfloat16)[:, None]
    send_rows = (jnp.take(tokens, slot_token, axis=0) * fill_rows).reshape(
        experts, capacity, width_local
    )
    send_words = jnp.take(words, slot_token, axis=0).reshape(experts, capacity, words.shape[1])
    recv_rows, recv_words = (
        lax.all_to_all(send_rows, "expert", split_axis=0, concat_axis=0, tiled=True),
        lax.all_to_all(send_words, "expert", split_axis=0, concat_axis=0, tiled=True),
    )
    rows = recv_rows.reshape(slots, width_local)
    recv_words = recv_words.reshape(slots, words.shape[1])
    input_signs = unpack_rows(recv_words[:, :sign_words])
    input_cols = unpack_cols(recv_words[:, :sign_words])
    signed = rows * input_signs.astype(jnp.bfloat16)
    mean_local = mean_weight[0]
    rho_float = rho_weight[0].astype(jnp.float32)
    noise_float = noise_weight[0].astype(jnp.float32)
    delta = (jax.nn.softplus(rho_float) * noise_float).astype(jnp.bfloat16)
    contract = (((0,), (1,)), ((), ()))
    output_cols = unpack_cols(recv_words[:, sign_words:])
    mean_cols = mean_local
    delta_cols = delta
    mean_part = lax.dot_general(mean_cols, rows, contract, preferred_element_type=jnp.float32)
    pert_part = lax.dot_general(delta_cols, signed, contract, preferred_element_type=jnp.float32)
    mean_part, pert_part = (mean_part, pert_part)
    preact = lax.psum_scatter(
        mean_part + output_cols * pert_part, "dp", scatter_dimension=0, tiled=True
    )
    gate = jax.nn.sigmoid(preact)
    hidden_slots = (preact * gate).astype(jnp.bfloat16)
    slope = gate * (1.0 + preact * (1.0 - gate))
    returned = lax.all_to_all(
        hidden_slots.reshape(hidden_local, experts, capacity),
        "expert",
        split_axis=1,
        concat_axis=1,
        tiled=True,
    )
    returned = returned.reshape(hidden_local, slots)
    picked = jnp.take(returned, slot_of, axis=1).astype(jnp.float32)
    hidden_out = jnp.sum(picked * route_weight[None], axis=2).T.astype(jnp.bfloat16)
    upstream = jnp.take(cotangent.T, slot_token, axis=1).astype(jnp.float32) * slot_weight[None, :]
    upstream = upstream.astype(jnp.bfloat16).reshape(hidden_local, experts, capacity)
    arrived = lax.all_to_all(upstream, "expert", split_axis=1, concat_axis=1, tiled=True).reshape(
        hidden_local, slots
    )
    grad_preact = (arrived.astype(jnp.float32) * slope).astype(jnp.bfloat16)
    piece = lax.all_gather(grad_preact, "dp", axis=0, tiled=True)
    piece_signed = piece * output_cols.astype(jnp.bfloat16)
    mean_cols = mean_local
    delta_cols = delta
    grad_rows = jnp.dot(mean_cols, piece, preferred_element_type=jnp.float32)
    grad_signed = jnp.dot(delta_cols, piece_signed, preferred_element_type=jnp.float32)
    mean_block = lax.dot_general(rows, piece, contract, preferred_element_type=jnp.float32)
    delta_block = lax.dot_general(
        signed, piece_signed, contract, preferred_element_type=jnp.float32
    )
    grad_mean_acc = mean_block
    grad_delta_acc = delta_block
    result = (grad_rows, grad_signed, grad_mean_acc, grad_delta_acc)
    grad_rows, grad_signed, grad_mean_acc, grad_delta_acc = result
    slot_grad = (grad_rows + input_cols * grad_signed).astype(jnp.bfloat16)
    back = lax.all_to_all(
        slot_grad.reshape(width_local, experts, capacity),
        "expert",
        split_axis=1,
        concat_axis=1,
        tiled=True,
    )
    back = back.reshape(width_local, slots)
    grad_tokens = jnp.sum(jnp.take(back, slot_of, axis=1).astype(jnp.float32), axis=2).T.astype(
        jnp.bfloat16
    )
    grad_mean = grad_mean_acc.astype(jnp.bfloat16)[None]
    grad_rho = (grad_delta_acc * noise_float * jax.nn.sigmoid(rho_float)).astype(jnp.bfloat16)[None]
    return (hidden_out, grad_tokens, grad_mean, grad_rho)


LANES = 128
VMEM_LIMIT = 56 * 1024 * 1024


def cost(flops, nbytes, trans=0):
    return pl.CostEstimate(flops=flops, bytes_accessed=nbytes, transcendentals=trans)


def params():
    return pltpu.CompilerParams(
        dimension_semantics=("arbitrary",), vmem_limit_bytes=VMEM_LIMIT
    )


def lane_signs(words, first, tiles):
    slots, total = words.shape
    lane = lax.broadcasted_iota(jnp.int32, (slots, LANES), 1)
    shift = lane % 32
    out = []
    for tile in range(tiles):
        at = first + 4 * tile + lane // 32
        picked = None
        for part in range(total // LANES):
            piece = jnp.take_along_axis(
                words[:, part * LANES : (part + 1) * LANES],
                at % LANES,
                axis=1,
                mode="promise_in_bounds",
            )
            picked = piece if part == 0 else jnp.where(at >= part * LANES, piece, picked)
        bits = jnp.bitwise_and(jnp.right_shift(picked, shift), 1)
        out.append((1 - 2 * bits).astype(jnp.float32))
    return jnp.concatenate(out, axis=1) if tiles > 1 else out[0]


def delta_kernel(rho_ref, noise_ref, delta_ref):
    rho = rho_ref[...].astype(jnp.float32)
    noise = noise_ref[...].astype(jnp.float32)
    soft = jnp.maximum(rho, 0.0) + jnp.log(1.0 + jnp.exp(-jnp.abs(rho)))
    delta_ref[...] = (soft * noise).astype(delta_ref.dtype)


def make_delta(rho, noise, rows=64):
    width, hidden = rho.shape
    spec = pl.BlockSpec((rows, hidden), lambda i: (i, 0))
    return pl.pallas_call(
        delta_kernel,
        grid=(width // rows,),
        in_specs=[spec, spec],
        out_specs=spec,
        out_shape=jax.ShapeDtypeStruct((width, hidden), jnp.bfloat16),
        compiler_params=params(),
        cost_estimate=cost(20 * width * hidden, 6 * width * hidden, 2 * width * hidden),
        name="delta",
    )(rho, noise)


def forward_kernel(in_words, words_ref, rows_ref, mean_ref, delta_ref, y_ref, r_ref, b_ref, s_ref):
    step = pl.program_id(0)
    block = mean_ref.shape[1]
    words = words_ref[...]

    @pl.when(step == 0)
    def _():
        signs = lane_signs(words, 0, rows_ref.shape[1] // LANES).astype(jnp.bfloat16)
        s_ref[...] = signs
        b_ref[...] = rows_ref[...] * signs

    signs = lane_signs(words, in_words + step * (block // 32), block // LANES)
    r_ref[0] = signs.astype(jnp.bfloat16)
    mean_part = jnp.dot(rows_ref[...], mean_ref[...], preferred_element_type=jnp.float32)
    pert_part = jnp.dot(b_ref[...], delta_ref[...], preferred_element_type=jnp.float32)
    y_ref[0] = (mean_part + signs * pert_part).astype(y_ref.dtype)


def forward(words, rows, mean, delta, parts, in_words):
    slots, width = rows.shape
    hidden = mean.shape[1]
    block = hidden // parts
    whole = lambda shape: pl.BlockSpec(shape, lambda i: (0, 0))
    weight = pl.BlockSpec((width, block), lambda i: (0, i))
    piece = pl.BlockSpec((1, slots, block), lambda i: (i, 0, 0))
    small = jax.ShapeDtypeStruct((slots, width), jnp.bfloat16)
    large = jax.ShapeDtypeStruct((parts, slots, block), jnp.bfloat16)
    return pl.pallas_call(
        functools.partial(forward_kernel, in_words),
        grid=(parts,),
        in_specs=[whole(words.shape), whole(rows.shape), weight, weight],
        out_specs=[piece, piece, whole(rows.shape), whole(rows.shape)],
        out_shape=[large, large, small, small],
        compiler_params=params(),
        cost_estimate=cost(4 * slots * width * hidden, 4 * hidden * (width + slots)),
        name="forward",
    )(words, rows, mean, delta)


NT = (((1,), (1,)), ((), ()))


def back_kernel(dy_ref, r_ref, mean_ref, delta_ref, s_ref, g_ref, plain, signed):
    step = pl.program_id(0)
    dy = dy_ref[0]
    one = lax.dot_general(dy, mean_ref[...], NT, preferred_element_type=jnp.float32)
    two = lax.dot_general(dy * r_ref[0], delta_ref[...], NT, preferred_element_type=jnp.float32)

    @pl.when(step == 0)
    def _():
        plain[...] = one
        signed[...] = two

    @pl.when(step > 0)
    def _():
        plain[...] += one
        signed[...] += two

    @pl.when(step == pl.num_programs(0) - 1)
    def _():
        total = plain[...] + s_ref[...].astype(jnp.float32) * signed[...]
        g_ref[...] = total.astype(g_ref.dtype)


def back(dy, r, mean, delta, s):
    parts, slots, block = dy.shape
    width = mean.shape[0]
    hidden = parts * block
    weight = pl.BlockSpec((width, block), lambda i: (0, i))
    piece = pl.BlockSpec((1, slots, block), lambda i: (i, 0, 0))
    whole = pl.BlockSpec((slots, width), lambda i: (0, 0))
    return pl.pallas_call(
        back_kernel,
        grid=(parts,),
        in_specs=[piece, piece, weight, weight, whole],
        out_specs=whole,
        out_shape=jax.ShapeDtypeStruct((slots, width), jnp.bfloat16),
        scratch_shapes=[pltpu.VMEM((slots, width), jnp.float32)] * 2,
        compiler_params=params(),
        cost_estimate=cost(4 * slots * width * hidden, 4 * hidden * (width + slots)),
        name="back",
    )(dy, r, mean, delta, s)


def grads_kernel(dy_ref, r_ref, rho_ref, noise_ref, at_ref, bt_ref, gm_ref, gr_ref):
    dy = dy_ref[0]
    gm = jnp.dot(at_ref[...], dy, preferred_element_type=jnp.float32)
    gm_ref[...] = gm.astype(gm_ref.dtype)
    gd = jnp.dot(bt_ref[...], dy * r_ref[0], preferred_element_type=jnp.float32)
    gate = 1.0 / (1.0 + jnp.exp(-rho_ref[...].astype(jnp.float32)))
    gr_ref[...] = (gd * noise_ref[...].astype(jnp.float32) * gate).astype(gr_ref.dtype)


def grads(dy, r, rho, noise, at, bt):
    parts, slots, block = dy.shape
    width, hidden = rho.shape
    weight = pl.BlockSpec((width, block), lambda i: (0, i))
    piece = pl.BlockSpec((1, slots, block), lambda i: (i, 0, 0))
    whole = pl.BlockSpec((width, slots), lambda i: (0, 0))
    out = jax.ShapeDtypeStruct((width, hidden), jnp.bfloat16)
    return pl.pallas_call(
        grads_kernel,
        grid=(parts,),
        in_specs=[piece, piece, weight, weight, whole, whole],
        out_specs=[weight, weight],
        out_shape=[out, out],
        compiler_params=params(),
        cost_estimate=cost(4 * slots * width * hidden, 8 * hidden * (width + slots)),
        name="grads",
    )(dy, r, rho, noise, at, bt)


def exact_dot(onehot, values):
    return jnp.dot(onehot, values, preferred_element_type=jnp.float32)


def on_device(
    tokens,
    in_signs,
    out_signs,
    expert_ids,
    route_weight,
    cotangent,
    mean_weight,
    rho_weight,
    noise_weight,
):
    parts = lax.axis_size("dp")
    hidden_local = cotangent.shape[1]
    width_local = tokens.shape[1]
    if hidden_local % LANES or width_local % LANES:
        return on_device_general(
            tokens,
            in_signs,
            out_signs,
            expert_ids,
            route_weight,
            cotangent,
            mean_weight,
            rho_weight,
            noise_weight,
        )
    experts = lax.axis_size("expert") * mean_weight.shape[0]
    token_count = tokens.shape[0]
    topk = expert_ids.shape[1]
    capacity = 5 * token_count * topk // (4 * experts)
    slots = experts * capacity
    in_words = in_signs.shape[1]
    mean, rho, noise = mean_weight[0], rho_weight[0], noise_weight[0]
    slot_of = block_slots(expert_ids, experts, capacity)
    match = slot_of[:, :, None] == jnp.arange(slots, dtype=jnp.int32)
    take_of = [match[:, k, :].astype(jnp.bfloat16) for k in range(topk)]
    fill_of = jnp.sum(match.astype(jnp.float32), axis=1).astype(jnp.bfloat16)
    slot_weight = jnp.sum(match.astype(jnp.float32) * route_weight[:, :, None], axis=(0, 1))
    token_rank = jnp.arange(token_count, dtype=jnp.int32)[:, None, None]
    slot_token = jnp.sum(match.astype(jnp.int32) * token_rank, axis=(0, 1))
    words = jnp.concatenate([in_signs, out_signs], axis=1)
    words = jnp.pad(words, ((0, 0), (0, -words.shape[1] % LANES)))
    send_words = jnp.take(words, slot_token, axis=0).reshape(experts, capacity, -1)
    fill_t = fill_of.T
    send_rows = exact_dot(fill_t, tokens).astype(jnp.bfloat16)
    upstream = (exact_dot(fill_t, cotangent) * slot_weight[:, None]).astype(jnp.bfloat16)
    swap = functools.partial(
        lax.all_to_all, axis_name="expert", split_axis=0, concat_axis=0, tiled=True
    )
    recv_rows = swap(send_rows.reshape(experts, capacity, -1)).reshape(slots, -1)
    recv_words = swap(send_words).reshape(slots, -1)
    arrived = swap(upstream.reshape(experts, capacity, -1)).reshape(slots, -1)
    delta = make_delta(rho, noise)
    partial, r, signed, s = forward(recv_words, recv_rows, mean, delta, parts, in_words)
    preact = lax.psum_scatter(partial, "dp", scatter_dimension=0, tiled=False)
    preact = preact.astype(jnp.float32)
    gate = jax.nn.sigmoid(preact)
    hidden_slots = (preact * gate).astype(jnp.bfloat16)
    slope = gate * (1.0 + preact * (1.0 - gate))
    dy = (arrived.astype(jnp.float32) * slope).astype(jnp.bfloat16)
    dy_all = lax.all_gather(dy, "dp", axis=0, tiled=False)
    returned = swap(hidden_slots.reshape(experts, capacity, -1)).reshape(slots, -1)
    hidden_out = sum(
        exact_dot(take_of[k], returned) * route_weight[:, k][:, None] for k in range(topk)
    ).astype(jnp.bfloat16)
    g = back(dy_all, r, mean, delta, s)
    g_back = swap(g.reshape(experts, capacity, -1)).reshape(slots, -1)
    grad_mean, grad_rho = grads(dy_all, r, rho, noise, recv_rows.T, signed.T)
    grad_tokens = exact_dot(fill_of, g_back).astype(jnp.bfloat16)
    return (hidden_out, grad_tokens, grad_mean[None], grad_rho[None])


def solution(mesh):
    in_specs = (
        P("expert", "dp"),
        P("expert", "dp"),
        P("expert", None),
        P("expert", None),
        P("expert", None),
        P("expert", "dp"),
        P("expert", "dp", None),
        P("expert", "dp", None),
        P("expert", "dp", None),
    )
    out_specs = (
        P("expert", "dp"),
        P("expert", "dp"),
        P("expert", "dp", None),
        P("expert", "dp", None),
    )
    return jax.shard_map(
        on_device, mesh=mesh, in_specs=in_specs, out_specs=out_specs, check_vma=False
    )
```

```python
import functools

import jax
import jax.numpy as jnp
from jax import lax
from jax.experimental import pallas as pl
from jax.experimental.pallas import tpu as pltpu
from jax.sharding import PartitionSpec as P

def unpack_rows(words):
    shifts = jnp.arange(32, dtype=jnp.int32)
    bits = jnp.bitwise_and(jnp.right_shift(words[..., None], shifts), 1)
    signs = (1 - 2 * bits).astype(jnp.float32)
    return signs.reshape(words.shape[:-1] + (words.shape[-1] * 32,))


def unpack_cols(words):
    shifts = jnp.arange(32, dtype=jnp.int32)
    bits = jnp.bitwise_and(jnp.right_shift(words.T[:, None, :], shifts[None, :, None]), 1)
    signs = (1 - 2 * bits).astype(jnp.float32)
    return signs.reshape(words.shape[1] * 32, words.shape[0])


def block_slots(block_ids, experts, capacity):
    onehot = (block_ids[:, :, None] == jnp.arange(experts, dtype=jnp.int32)).astype(jnp.int32)
    flat = onehot.reshape(-1, experts)
    before = jnp.cumsum(flat, axis=0) - flat
    ranks = jnp.sum(before * flat, axis=1).reshape(block_ids.shape)
    return block_ids * capacity + ranks


def on_device_general(
    tokens,
    in_signs,
    out_signs,
    expert_ids,
    route_weight,
    cotangent,
    mean_weight,
    rho_weight,
    noise_weight,
):
    experts = lax.axis_size("expert") * mean_weight.shape[0]
    token_count = tokens.shape[0]
    topk = expert_ids.shape[1]
    capacity = 5 * token_count * topk // (4 * experts)
    slots = experts * capacity
    width_local = tokens.shape[1]
    sign_words = in_signs.shape[1]
    hidden_local = cotangent.shape[1]
    slot_of = block_slots(expert_ids, experts, capacity)
    match = (slot_of[:, :, None] == jnp.arange(slots, dtype=jnp.int32)).astype(jnp.int32)
    token_rank = jnp.arange(token_count, dtype=jnp.int32)[:, None, None]
    slot_token = jnp.sum(match * token_rank, axis=(0, 1))
    slot_fill = jnp.sum(match, axis=(0, 1))
    slot_weight = jnp.sum(match.astype(jnp.float32) * route_weight[:, :, None], axis=(0, 1))
    words = jnp.concatenate([in_signs, out_signs], axis=1)
    fill_rows = slot_fill.astype(jnp.bfloat16)[:, None]
    send_rows = (jnp.take(tokens, slot_token, axis=0) * fill_rows).reshape(
        experts, capacity, width_local
    )
    send_words = jnp.take(words, slot_token, axis=0).reshape(experts, capacity, words.shape[1])
    recv_rows, recv_words = (
        lax.all_to_all(send_rows, "expert", split_axis=0, concat_axis=0, tiled=True),
        lax.all_to_all(send_words, "expert", split_axis=0, concat_axis=0, tiled=True),
    )
    rows = recv_rows.reshape(slots, width_local)
    recv_words = recv_words.reshape(slots, words.shape[1])
    input_signs = unpack_rows(recv_words[:, :sign_words])
    input_cols = unpack_cols(recv_words[:, :sign_words])
    signed = rows * input_signs.astype(jnp.bfloat16)
    mean_local = mean_weight[0]
    rho_float = rho_weight[0].astype(jnp.float32)
    noise_float = noise_weight[0].astype(jnp.float32)
    delta = (jax.nn.softplus(rho_float) * noise_float).astype(jnp.bfloat16)
    contract = (((0,), (1,)), ((), ()))
    output_cols = unpack_cols(recv_words[:, sign_words:])
    mean_cols = mean_local
    delta_cols = delta
    mean_part = lax.dot_general(mean_cols, rows, contract, preferred_element_type=jnp.float32)
    pert_part = lax.dot_general(delta_cols, signed, contract, preferred_element_type=jnp.float32)
    mean_part, pert_part = (mean_part, pert_part)
    preact = lax.psum_scatter(
        mean_part + output_cols * pert_part, "dp", scatter_dimension=0, tiled=True
    )
    gate = jax.nn.sigmoid(preact)
    hidden_slots = (preact * gate).astype(jnp.bfloat16)
    slope = gate * (1.0 + preact * (1.0 - gate))
    returned = lax.all_to_all(
        hidden_slots.reshape(hidden_local, experts, capacity),
        "expert",
        split_axis=1,
        concat_axis=1,
        tiled=True,
    )
    returned = returned.reshape(hidden_local, slots)
    picked = jnp.take(returned, slot_of, axis=1).astype(jnp.float32)
    hidden_out = jnp.sum(picked * route_weight[None], axis=2).T.astype(jnp.bfloat16)
    upstream = jnp.take(cotangent.T, slot_token, axis=1).astype(jnp.float32) * slot_weight[None, :]
    upstream = upstream.astype(jnp.bfloat16).reshape(hidden_local, experts, capacity)
    arrived = lax.all_to_all(upstream, "expert", split_axis=1, concat_axis=1, tiled=True).reshape(
        hidden_local, slots
    )
    grad_preact = (arrived.astype(jnp.float32) * slope).astype(jnp.bfloat16)
    piece = lax.all_gather(grad_preact, "dp", axis=0, tiled=True)
    piece_signed = piece * output_cols.astype(jnp.bfloat16)
    mean_cols = mean_local
    delta_cols = delta
    grad_rows = jnp.dot(mean_cols, piece, preferred_element_type=jnp.float32)
    grad_signed = jnp.dot(delta_cols, piece_signed, preferred_element_type=jnp.float32)
    mean_block = lax.dot_general(rows, piece, contract, preferred_element_type=jnp.float32)
    delta_block = lax.dot_general(
        signed, piece_signed, contract, preferred_element_type=jnp.float32
    )
    grad_mean_acc = mean_block
    grad_delta_acc = delta_block
    result = (grad_rows, grad_signed, grad_mean_acc, grad_delta_acc)
    grad_rows, grad_signed, grad_mean_acc, grad_delta_acc = result
    slot_grad = (grad_rows + input_cols * grad_signed).astype(jnp.bfloat16)
    back = lax.all_to_all(
        slot_grad.reshape(width_local, experts, capacity),
        "expert",
        split_axis=1,
        concat_axis=1,
        tiled=True,
    )
    back = back.reshape(width_local, slots)
    grad_tokens = jnp.sum(jnp.take(back, slot_of, axis=1).astype(jnp.float32), axis=2).T.astype(
        jnp.bfloat16
    )
    grad_mean = grad_mean_acc.astype(jnp.bfloat16)[None]
    grad_rho = (grad_delta_acc * noise_float * jax.nn.sigmoid(rho_float)).astype(jnp.bfloat16)[None]
    return (hidden_out, grad_tokens, grad_mean, grad_rho)


LANES = 128
VMEM_LIMIT = 56 * 1024 * 1024


def cost(flops, nbytes, trans=0):
    return pl.CostEstimate(flops=flops, bytes_accessed=nbytes, transcendentals=trans)


def params():
    return pltpu.CompilerParams(
        dimension_semantics=("arbitrary",), vmem_limit_bytes=VMEM_LIMIT
    )


def lane_signs(words, first, tiles):
    slots, total = words.shape
    lane = lax.broadcasted_iota(jnp.int32, (slots, LANES), 1)
    shift = lane % 32
    out = []
    for tile in range(tiles):
        at = first + 4 * tile + lane // 32
        picked = None
        for part in range(total // LANES):
            piece = jnp.take_along_axis(
                words[:, part * LANES : (part + 1) * LANES],
                at % LANES,
                axis=1,
                mode="promise_in_bounds",
            )
            picked = piece if part == 0 else jnp.where(at >= part * LANES, piece, picked)
        bits = jnp.bitwise_and(jnp.right_shift(picked, shift), 1)
        out.append((1 - 2 * bits).astype(jnp.float32))
    return jnp.concatenate(out, axis=1) if tiles > 1 else out[0]


def delta_kernel(rho_ref, noise_ref, delta_ref):
    rho = rho_ref[...].astype(jnp.float32)
    noise = noise_ref[...].astype(jnp.float32)
    soft = jnp.maximum(rho, 0.0) + jnp.log(1.0 + jnp.exp(-jnp.abs(rho)))
    delta_ref[...] = (soft * noise).astype(delta_ref.dtype)


def make_delta(rho, noise, rows=64):
    width, hidden = rho.shape
    spec = pl.BlockSpec((rows, hidden), lambda i: (i, 0))
    return pl.pallas_call(
        delta_kernel,
        grid=(width // rows,),
        in_specs=[spec, spec],
        out_specs=spec,
        out_shape=jax.ShapeDtypeStruct((width, hidden), jnp.bfloat16),
        compiler_params=params(),
        cost_estimate=cost(20 * width * hidden, 6 * width * hidden, 2 * width * hidden),
        name="delta",
    )(rho, noise)


def forward_kernel(in_words, words_ref, rows_ref, mean_ref, delta_ref, y_ref, r_ref, b_ref, s_ref):
    step = pl.program_id(0)
    block = mean_ref.shape[1]
    words = words_ref[...]

    @pl.when(step == 0)
    def _():
        signs = lane_signs(words, 0, rows_ref.shape[1] // LANES).astype(jnp.bfloat16)
        s_ref[...] = signs
        b_ref[...] = rows_ref[...] * signs

    signs = lane_signs(words, in_words + step * (block // 32), block // LANES)
    r_ref[0] = signs.astype(jnp.bfloat16)
    mean_part = jnp.dot(rows_ref[...], mean_ref[...], preferred_element_type=jnp.float32)
    pert_part = jnp.dot(b_ref[...], delta_ref[...], preferred_element_type=jnp.float32)
    y_ref[0] = (mean_part + signs * pert_part).astype(y_ref.dtype)


def forward(words, rows, mean, delta, parts, in_words):
    slots, width = rows.shape
    hidden = mean.shape[1]
    block = hidden // parts
    whole = lambda shape: pl.BlockSpec(shape, lambda i: (0, 0))
    weight = pl.BlockSpec((width, block), lambda i: (0, i))
    piece = pl.BlockSpec((1, slots, block), lambda i: (i, 0, 0))
    small = jax.ShapeDtypeStruct((slots, width), jnp.bfloat16)
    large = jax.ShapeDtypeStruct((parts, slots, block), jnp.bfloat16)
    return pl.pallas_call(
        functools.partial(forward_kernel, in_words),
        grid=(parts,),
        in_specs=[whole(words.shape), whole(rows.shape), weight, weight],
        out_specs=[piece, piece, whole(rows.shape), whole(rows.shape)],
        out_shape=[large, large, small, small],
        compiler_params=params(),
        cost_estimate=cost(4 * slots * width * hidden, 4 * hidden * (width + slots)),
        name="forward",
    )(words, rows, mean, delta)


NT = (((1,), (1,)), ((), ()))


def back_kernel(dy_ref, r_ref, mean_ref, delta_ref, s_ref, g_ref, plain, signed):
    step = pl.program_id(0)
    dy = dy_ref[0]
    one = lax.dot_general(dy, mean_ref[...], NT, preferred_element_type=jnp.float32)
    two = lax.dot_general(dy * r_ref[0], delta_ref[...], NT, preferred_element_type=jnp.float32)

    @pl.when(step == 0)
    def _():
        plain[...] = one
        signed[...] = two

    @pl.when(step > 0)
    def _():
        plain[...] += one
        signed[...] += two

    @pl.when(step == pl.num_programs(0) - 1)
    def _():
        total = plain[...] + s_ref[...].astype(jnp.float32) * signed[...]
        g_ref[...] = total.astype(g_ref.dtype)


def back(dy, r, mean, delta, s):
    parts, slots, block = dy.shape
    width = mean.shape[0]
    hidden = parts * block
    weight = pl.BlockSpec((width, block), lambda i: (0, i))
    piece = pl.BlockSpec((1, slots, block), lambda i: (i, 0, 0))
    whole = pl.BlockSpec((slots, width), lambda i: (0, 0))
    return pl.pallas_call(
        back_kernel,
        grid=(parts,),
        in_specs=[piece, piece, weight, weight, whole],
        out_specs=whole,
        out_shape=jax.ShapeDtypeStruct((slots, width), jnp.bfloat16),
        scratch_shapes=[pltpu.VMEM((slots, width), jnp.float32)] * 2,
        compiler_params=params(),
        cost_estimate=cost(4 * slots * width * hidden, 4 * hidden * (width + slots)),
        name="back",
    )(dy, r, mean, delta, s)


def grads_kernel(dy_ref, r_ref, rho_ref, noise_ref, at_ref, bt_ref, gm_ref, gr_ref):
    dy = dy_ref[0]
    gm = jnp.dot(at_ref[...], dy, preferred_element_type=jnp.float32)
    gm_ref[...] = gm.astype(gm_ref.dtype)
    gd = jnp.dot(bt_ref[...], dy * r_ref[0], preferred_element_type=jnp.float32)
    gate = 1.0 / (1.0 + jnp.exp(-rho_ref[...].astype(jnp.float32)))
    gr_ref[...] = (gd * noise_ref[...].astype(jnp.float32) * gate).astype(gr_ref.dtype)


def grads(dy, r, rho, noise, at, bt):
    parts, slots, block = dy.shape
    width, hidden = rho.shape
    weight = pl.BlockSpec((width, block), lambda i: (0, i))
    piece = pl.BlockSpec((1, slots, block), lambda i: (i, 0, 0))
    whole = pl.BlockSpec((width, slots), lambda i: (0, 0))
    out = jax.ShapeDtypeStruct((width, hidden), jnp.bfloat16)
    return pl.pallas_call(
        grads_kernel,
        grid=(parts,),
        in_specs=[piece, piece, weight, weight, whole, whole],
        out_specs=[weight, weight],
        out_shape=[out, out],
        compiler_params=params(),
        cost_estimate=cost(4 * slots * width * hidden, 8 * hidden * (width + slots)),
        name="grads",
    )(dy, r, rho, noise, at, bt)


def exchange_kernel(
    p_ref, up_ref, out_ref, back_ref, arr, rd, cs, ra, rb, rc, h_ref, send_sem, recv_sem
):
    me = lax.axis_index("dp")
    mine = lax.axis_index("expert")
    ranks = up_ref.shape[0]
    cap = up_ref.shape[1]
    half = p_ref.shape[1] // 2
    y, x, c = me // 4, (me // 2) % 2, me % 2
    place = lambda dy, dx, dc: ((y + dy) % 2) * 4 + ((x + dx) % 2) * 2 + (c + dc) % 2
    at_x, at_y, at_c = place(0, 1, 0), place(1, 0, 0), place(0, 0, 1)
    rows = [pl.ds(0, half), pl.ds(half, half)]
    peers = [(at_x, mine), (at_y, mine), (at_c, mine)]
    peers += [(me, (mine + j) % ranks) for j in range(1, ranks)]
    count = [0]
    started = []

    def send(src, dst, to):
        n = count[0]
        count[0] += 1
        copy = pltpu.make_async_remote_copy(
            src_ref=src,
            dst_ref=dst,
            send_sem=send_sem.at[n],
            recv_sem=recv_sem.at[n],
            device_id=to,
            device_id_type=pl.DeviceIdType.MESH,
        )
        copy.start()
        started.append(copy)
        return copy

    barrier = pltpu.get_barrier_semaphore()
    for peer in peers:
        pl.semaphore_signal(barrier, inc=1, device_id=peer, device_id_type=pl.DeviceIdType.MESH)
    pl.semaphore_wait(barrier, len(peers))

    order = (3, 1, 2, 0)
    core = {
        k: send(p_ref.at[place(k // 2, k % 2, 1)], rd.at[k], (at_c, mine)) for k in order
    }
    to_owner = [
        send(up_ref.at[(mine + j) % ranks], arr.at[mine], (me, (mine + j) % ranks))
        for j in range(1, ranks)
    ]
    arr[mine] = up_ref[mine]

    def add(*terms):
        total = terms[0].astype(jnp.float32)
        for term in terms[1:]:
            total = total + term.astype(jnp.float32)
        return total

    def chip_sum(k, which):
        at = rows[which]
        cs[k, at] = add(p_ref[place(k // 2, k % 2, 0), at], rd[k, at]).astype(cs.dtype)

    core[3].wait_recv()
    chip_sum(3, 0)
    along_x = [send(cs.at[3, rows[0]], ra.at[1], (at_x, mine))]
    chip_sum(3, 1)
    along_y = [send(cs.at[3, rows[1]], rb.at[1], (at_y, mine))]
    core[1].wait_recv()
    chip_sum(1, 0)
    along_x.append(send(cs.at[1, rows[0]], ra.at[0], (at_x, mine)))
    core[2].wait_recv()
    chip_sum(2, 1)
    along_y.append(send(cs.at[2, rows[1]], rb.at[0], (at_y, mine)))
    along_x[0].wait_recv()
    at = rows[0]
    cs[2, at] = add(p_ref[place(1, 0, 0), at], rd[2, at], ra[1]).astype(cs.dtype)
    last_y = send(cs.at[2, at], rc.at[0], (at_y, mine))
    along_y[0].wait_recv()
    at = rows[1]
    cs[1, at] = add(p_ref[place(0, 1, 0), at], rd[1, at], rb[1]).astype(cs.dtype)
    last_x = send(cs.at[1, at], rc.at[1], (at_x, mine))
    core[0].wait_recv()
    for copy in to_owner:
        copy.wait_recv()

    def activate(which, near):
        per = ranks // 2
        for i in range(per):
            own = pl.ds(which * half + i * cap, cap)
            part = pl.ds(i * cap, cap)
            preact = add(p_ref[me, own], rd[0, own], near[0, part], rc[which, part])
            gate = 1.0 / (1.0 + jnp.exp(-preact))
            h_ref[which * per + i] = (preact * gate).astype(h_ref.dtype)
            slope = gate * (1.0 + preact * (1.0 - gate))
            up = arr[which * per + i].astype(jnp.float32)
            out_ref[me, own] = (up * slope).astype(out_ref.dtype)

    def spread(owner, which, to):
        piece = out_ref.at[owner, rows[which]]
        return send(piece, piece, (to, mine))

    along_x[1].wait_recv()
    last_y.wait_recv()
    activate(0, ra)
    y_one = spread(me, 0, at_y)
    x_two = spread(me, 0, at_x)
    c_all = [spread(me, 0, at_c)]
    along_y[1].wait_recv()
    last_x.wait_recv()
    activate(1, rb)
    x_one = spread(me, 1, at_x)
    y_two = spread(me, 1, at_y)
    c_all.append(spread(me, 1, at_c))
    to_token = [
        send(h_ref.at[(mine + j) % ranks], back_ref.at[mine], (me, (mine + j) % ranks))
        for j in range(1, ranks)
    ]
    back_ref[mine] = h_ref[mine]
    y_one.wait_recv()
    x_three = spread(at_y, 0, at_x)
    c_all.append(spread(at_y, 0, at_c))
    x_one.wait_recv()
    y_three = spread(at_x, 1, at_y)
    c_all.append(spread(at_x, 1, at_c))
    x_two.wait_recv()
    c_all.append(spread(at_x, 0, at_c))
    y_two.wait_recv()
    c_all.append(spread(at_y, 1, at_c))
    x_three.wait_recv()
    c_all.append(spread(place(1, 1, 0), 0, at_c))
    y_three.wait_recv()
    c_all.append(spread(place(1, 1, 0), 1, at_c))
    for copy in c_all + to_token:
        copy.wait_recv()
    for copy in started:
        copy.wait_send()


def exchange(partial, upstream):
    parts, slots, block = partial.shape
    ranks, cap, _ = upstream.shape
    bf16 = jnp.bfloat16
    vmem = pl.BlockSpec(memory_space=pltpu.VMEM)
    copies = 4 + 4 + 2 + 6 + 8 + 2 * (ranks - 1)
    half = (2, slots // 2, block)
    return pl.pallas_call(
        exchange_kernel,
        in_specs=[vmem, vmem],
        out_specs=[vmem, vmem],
        out_shape=[
            jax.ShapeDtypeStruct(partial.shape, bf16),
            jax.ShapeDtypeStruct(upstream.shape, bf16),
        ],
        scratch_shapes=[
            pltpu.VMEM(upstream.shape, bf16),
            pltpu.VMEM((4, slots, block), bf16),
            pltpu.VMEM((4, slots, block), bf16),
            pltpu.VMEM(half, bf16),
            pltpu.VMEM(half, bf16),
            pltpu.VMEM(half, bf16),
            pltpu.VMEM(upstream.shape, bf16),
            pltpu.SemaphoreType.DMA((copies,)),
            pltpu.SemaphoreType.DMA((copies,)),
        ],
        compiler_params=pltpu.CompilerParams(
            collective_id=0, has_side_effects=True, vmem_limit_bytes=VMEM_LIMIT
        ),
        cost_estimate=cost(10 * partial.size, 100 * partial.size),
        name="exchange",
    )(partial, upstream)


def exact_dot(onehot, values):
    return jnp.dot(onehot, values, preferred_element_type=jnp.float32)


def on_device(
    tokens,
    in_signs,
    out_signs,
    expert_ids,
    route_weight,
    cotangent,
    mean_weight,
    rho_weight,
    noise_weight,
):
    parts = lax.axis_size("dp")
    token_count = tokens.shape[0]
    hidden_local = cotangent.shape[1]
    width_local = tokens.shape[1]
    ranks = lax.axis_size("expert")
    fits = parts == 8 and ranks % 2 == 0 and mean_weight.shape[0] == 1
    if not fits or hidden_local % LANES or width_local % LANES or token_count % 128:
        return on_device_general(
            tokens,
            in_signs,
            out_signs,
            expert_ids,
            route_weight,
            cotangent,
            mean_weight,
            rho_weight,
            noise_weight,
        )
    experts = ranks
    topk = expert_ids.shape[1]
    capacity = 5 * token_count * topk // (4 * experts)
    slots = experts * capacity
    in_words = in_signs.shape[1]
    mean, rho, noise = mean_weight[0], rho_weight[0], noise_weight[0]
    slot_of = block_slots(expert_ids, experts, capacity)
    match = slot_of[:, :, None] == jnp.arange(slots, dtype=jnp.int32)
    take_of = [match[:, k, :].astype(jnp.bfloat16) for k in range(topk)]
    fill_of = jnp.sum(match.astype(jnp.float32), axis=1).astype(jnp.bfloat16)
    slot_weight = jnp.sum(match.astype(jnp.float32) * route_weight[:, :, None], axis=(0, 1))
    token_rank = jnp.arange(token_count, dtype=jnp.int32)[:, None, None]
    slot_token = jnp.sum(match.astype(jnp.int32) * token_rank, axis=(0, 1))
    words = jnp.concatenate([in_signs, out_signs], axis=1)
    words = jnp.pad(words, ((0, 0), (0, -words.shape[1] % LANES)))
    send_words = jnp.take(words, slot_token, axis=0).reshape(experts, capacity, -1)
    fill_t = fill_of.T
    send_rows = exact_dot(fill_t, tokens).astype(jnp.bfloat16)
    upstream = (exact_dot(fill_t, cotangent) * slot_weight[:, None]).astype(jnp.bfloat16)
    swap = functools.partial(
        lax.all_to_all, axis_name="expert", split_axis=0, concat_axis=0, tiled=True
    )
    recv_rows = swap(send_rows.reshape(experts, capacity, -1)).reshape(slots, -1)
    recv_words = swap(send_words).reshape(slots, -1)
    delta = make_delta(rho, noise)
    partial, r, signed, s = forward(recv_words, recv_rows, mean, delta, parts, in_words)
    dy_all, returned = exchange(partial, upstream.reshape(experts, capacity, -1))
    returned = returned.reshape(slots, -1)
    hidden_out = sum(
        exact_dot(take_of[k], returned) * route_weight[:, k][:, None] for k in range(topk)
    ).astype(jnp.bfloat16)
    g = back(dy_all, r, mean, delta, s)
    g_back = swap(g.reshape(experts, capacity, -1)).reshape(slots, -1)
    grad_mean, grad_rho = grads(dy_all, r, rho, noise, recv_rows.T, signed.T)
    grad_tokens = exact_dot(fill_of, g_back).astype(jnp.bfloat16)
    return (hidden_out, grad_tokens, grad_mean[None], grad_rho[None])


def solution(mesh):
    in_specs = (
        P("expert", "dp"),
        P("expert", "dp"),
        P("expert", None),
        P("expert", None),
        P("expert", None),
        P("expert", "dp"),
        P("expert", "dp", None),
        P("expert", "dp", None),
        P("expert", "dp", None),
    )
    out_specs = (
        P("expert", "dp"),
        P("expert", "dp"),
        P("expert", "dp", None),
        P("expert", "dp", None),
    )
    return jax.shard_map(
        on_device, mesh=mesh, in_specs=in_specs, out_specs=out_specs, check_vma=False
    )
```
